32 devices in a mesh: data: 4 (over y, z), model: 8 (over x, core).
Axes of the slice: x: 4, y: 2, z: 2, core: 2. Of those that a mesh axis runs over, the one named last changes fastest.
The devices are a block of a 4x4x8 slice.
Arguments:
- x_tok: bfloat16 [8, 1024, 4096], P('data', 'model'), parts along dimension 0
- dy_tok: bfloat16 [8, 1024, 4096], P('data', 'model'), parts along dimension 0
- w_q: bfloat16 [4096, 32, 128], P(None, 'model')
- w_k: bfloat16 [4096, 2, 128], replicated
- w_v: bfloat16 [4096, 2, 128], replicated
- w_o: bfloat16 [32, 128, 4096], P('model')
Outputs:
- output 1: bfloat16 [8, 1024, 4096], P('data', 'model'), parts along dimension 0
- output 2: float32 [16384, 32, 128], P('data', 'model'), parts along dimension 0
- output 3: float32 [32768, 128], P(('data', 'model')), parts along dimension 0
- output 4: float32 [32768, 128], P(('data', 'model')), parts along dimension 0
- output 5: float32 [128, 128, 4096], P(('data', 'model')), parts along dimension 0
There are 4 independent parts. The reference program is written for one: setup_inputs(seed, part) draws one part's arguments, and reference() takes and returns one part's arrays. A program takes and returns all parts, laid end to end along the dimension named above; an argument that names none is the same for every part.
All inputs are finite; a program needn't handle non-finite values.
Results may differ from the reference program's by a relative error of at most 0.00886.
Values are sent between devices in bfloat16 or wider.
A program may use at most 768 MiB of HBM per device.

```python
import jax
import jax.numpy as jnp
from jax import lax

D = 4096
HEADS = 32
KV_HEADS = 2
HEAD = 128
SEQ = 1024
MICRO = 2

GROUP_HEADS = HEADS // KV_HEADS
SCORE_SCALE = HEAD ** -0.5


def setup_inputs(seed: int = 0, part: int = 0) -> dict:
    part_key = jax.random.fold_in(jax.random.key(seed), part)
    key_x, key_dy = jax.random.split(part_key, 2)
    key_q, key_k, key_v, key_o = jax.random.split(jax.random.key(seed + 1), 4)
    x_tok = jax.random.normal(key_x, (MICRO, SEQ, D), jnp.float32).astype(jnp.bfloat16)
    dy_tok = jax.random.normal(key_dy, (MICRO, SEQ, D), jnp.float32).astype(jnp.bfloat16)
    w_q = (jax.random.normal(key_q, (D, HEADS, HEAD), jnp.float32) * D ** -0.5).astype(jnp.bfloat16)
    w_k = (jax.random.normal(key_k, (D, KV_HEADS, HEAD), jnp.float32) * D ** -0.5).astype(jnp.bfloat16)
    w_v = (jax.random.normal(key_v, (D, KV_HEADS, HEAD), jnp.float32) * D ** -0.5).astype(jnp.bfloat16)
    w_o = (jax.random.normal(key_o, (HEADS, HEAD, D), jnp.float32) * (HEADS * HEAD) ** -0.5).astype(jnp.bfloat16)
    return {"x_tok": x_tok, "dy_tok": dy_tok, "w_q": w_q, "w_k": w_k, "w_v": w_v, "w_o": w_o}


def micro_grads(micro_in, w_q, w_k, w_v, w_o):
    x_micro, dy_micro = micro_in
    w_q_flat = w_q.reshape(D, HEADS * HEAD)
    w_k_flat = w_k.reshape(D, KV_HEADS * HEAD)
    w_v_flat = w_v.reshape(D, KV_HEADS * HEAD)
    w_o_flat = w_o.reshape(HEADS * HEAD, D)
    q_all = jnp.dot(x_micro, w_q_flat, preferred_element_type=jnp.float32).astype(jnp.bfloat16).reshape(SEQ, HEADS, HEAD)
    k_all = jnp.dot(x_micro, w_k_flat, preferred_element_type=jnp.float32).astype(jnp.bfloat16).reshape(SEQ, KV_HEADS, HEAD)
    v_all = jnp.dot(x_micro, w_v_flat, preferred_element_type=jnp.float32).astype(jnp.bfloat16).reshape(SEQ, KV_HEADS, HEAD)
    d_out = jnp.dot(dy_micro, w_o_flat.T, preferred_element_type=jnp.float32).astype(jnp.bfloat16).reshape(SEQ, HEADS, HEAD)
    k_rep = jnp.repeat(k_all, GROUP_HEADS, axis=1)
    v_rep = jnp.repeat(v_all, GROUP_HEADS, axis=1)
    q_pos = jnp.arange(SEQ)[:, None]
    k_pos = jnp.arange(SEQ)[None, :]

    def head_grads(head_in):
        q_head, k_head, v_head, do_head = head_in
        scores = jnp.dot(q_head, k_head.T, preferred_element_type=jnp.float32) * SCORE_SCALE
        scores = jnp.where(q_pos >= k_pos, scores, -jnp.inf)
        prob_f32 = jax.nn.softmax(scores, axis=-1)
        prob_b16 = prob_f32.astype(jnp.bfloat16)
        out_head = jnp.dot(prob_b16, v_head, preferred_element_type=jnp.float32).astype(jnp.bfloat16)
        d_prob = jnp.dot(do_head, v_head.T, preferred_element_type=jnp.float32)
        row_delta = jnp.sum(do_head.astype(jnp.float32) * out_head.astype(jnp.float32), axis=-1, keepdims=True)
        d_score = (prob_f32 * (d_prob - row_delta)).astype(jnp.bfloat16)
        dq_head = (jnp.dot(d_score, k_head, preferred_element_type=jnp.float32) * SCORE_SCALE).astype(jnp.bfloat16)
        dk_head = jnp.dot(d_score.T, q_head, preferred_element_type=jnp.float32) * SCORE_SCALE
        dv_head = jnp.dot(prob_b16.T, do_head, preferred_element_type=jnp.float32)
        dwo_head = jnp.dot(out_head.T, dy_micro, preferred_element_type=jnp.float32)
        return dq_head, dk_head, dv_head, dwo_head

    heads_major = (q_all.transpose(1, 0, 2), k_rep.transpose(1, 0, 2), v_rep.transpose(1, 0, 2), d_out.transpose(1, 0, 2))
    d_q, d_k, d_v, dw_o = lax.map(head_grads, heads_major)
    d_k_sum = d_k.reshape(KV_HEADS, GROUP_HEADS, SEQ, HEAD).sum(axis=1).astype(jnp.bfloat16)
    d_v_sum = d_v.reshape(KV_HEADS, GROUP_HEADS, SEQ, HEAD).sum(axis=1).astype(jnp.bfloat16)
    d_q_flat = d_q.transpose(1, 0, 2).reshape(SEQ, HEADS * HEAD)
    d_k_flat = d_k_sum.transpose(1, 0, 2).reshape(SEQ, KV_HEADS * HEAD)
    d_v_flat = d_v_sum.transpose(1, 0, 2).reshape(SEQ, KV_HEADS * HEAD)
    dw_q = jnp.dot(x_micro.T, d_q_flat, preferred_element_type=jnp.float32).reshape(D, HEADS, HEAD)
    dw_k = jnp.dot(x_micro.T, d_k_flat, preferred_element_type=jnp.float32).reshape(D, KV_HEADS, HEAD)
    dw_v = jnp.dot(x_micro.T, d_v_flat, preferred_element_type=jnp.float32).reshape(D, KV_HEADS, HEAD)
    dx_f32 = (jnp.dot(d_q_flat, w_q_flat.T, preferred_element_type=jnp.float32)
              + jnp.dot(d_k_flat, w_k_flat.T, preferred_element_type=jnp.float32)
              + jnp.dot(d_v_flat, w_v_flat.T, preferred_element_type=jnp.float32))
    return dx_f32.astype(jnp.bfloat16), dw_q, dw_k, dw_v, dw_o


def reference(x_tok, dy_tok, w_q, w_k, w_v, w_o):
    def one_micro(micro_in):
        return micro_grads(micro_in, w_q, w_k, w_v, w_o)

    dx_tok, dw_q, dw_k, dw_v, dw_o = lax.map(one_micro, (x_tok, dy_tok))
    dw_k_rows = dw_k.sum(axis=0).transpose(1, 0, 2).reshape(KV_HEADS * D, HEAD)
    dw_v_rows = dw_v.sum(axis=0).transpose(1, 0, 2).reshape(KV_HEADS * D, HEAD)
    return (dx_tok, dw_q.sum(axis=0), dw_k_rows, dw_v_rows, dw_o.sum(axis=0))
```

```python
import functools

import jax
import jax.numpy as jnp
from jax import lax
from jax.experimental import pallas as pl
from jax.experimental.pallas import tpu as pltpu
from jax.sharding import PartitionSpec as P

F32 = jnp.float32
BF16 = jnp.bfloat16
NT = (((1,), (1,)), ((), ()))
TN = (((0,), (0,)), ((), ()))
CORES = 2
RIGHT, LEFT = 0, 1
MESH = pl.DeviceIdType.MESH


def fused_kernel(chips, heads, hd, x_in, y_in, wcat_in, wo_in,
                 xg, yg, dqkv_out, o_out, dx_out, snd_out, keep_out,
                 wcat, wo, nat, donat, dnat, onat, dk_acc, dv_acc, xbuf, lhs, gsum,
                 mate_stage, mate_recv, rs_send, rs_recv, dx_buf, snd_buf,
                 ring_s, ring_r, core_s, core_r, mate_s, mate_r, own_sem, w_sem, in_sem, out_sem):
    micro_n, tok, d = x_in.shape
    h2 = tok // 2
    n = chips * CORES
    qw = heads * hd
    wide = qw + 2 * hd
    seq = n * tok
    me = lax.axis_index("model")
    chip, core = me // CORES, lax.rem(me, CORES)
    to_right, to_left = lax.rem(me + CORES, n), lax.rem(me + n - CORES, n)
    mate = chip * CORES + 1 - core
    scale = hd ** -0.5

    def chip_at(s):
        return lax.rem(chip + s, chips)

    def block(s, q):
        return (chip_at(s) * CORES + q) * tok

    def rows(ref, i, s, q, off, size):
        return ref.at[i, pl.ds(pl.multiple_of(block(s, q) + off, h2), size), :]

    def remote(src, dst, s_sem, r_sem, dev):
        return pltpu.make_async_remote_copy(src_ref=src, dst_ref=dst, send_sem=s_sem, recv_sem=r_sem,
                                            device_id={"model": dev}, device_id_type=MESH)

    barrier = pltpu.get_barrier_semaphore()
    for dev in (to_right, to_left, mate):
        pl.semaphore_signal(barrier, inc=1, device_id={"model": dev}, device_id_type=MESH)
    pl.semaphore_wait(barrier, 3)

    tensors = []
    for i in range(micro_n):
        tensors += [(i, x_in, xg), (i, y_in, yg)]
    n_gather = 3 * len(tensors)

    def ring_copies(k):
        sems = [(ring_s.at[k, e], ring_r.at[k, e]) for e in range(2)]
        if k < n_gather:
            i, src, g = tensors[k // 3]
            part = k % 3
            if part < 2:
                offs = (part * h2, (1 - part) * h2)
                srcs = [src.at[i, pl.ds(off, h2), :] for off in offs]
                dsts = [rows(g, i, 0, core, off, h2) for off in offs]
            else:
                srcs = dsts = [rows(g, i, chips - 1, core, 0, h2), rows(g, i, 1, core, h2, h2)]
        else:
            srcs = [rs_send.at[k - n_gather, e] for e in range(2)]
            dsts = [rs_recv.at[k - n_gather, e] for e in range(2)]
        return [remote(srcs[e], dsts[e], *sems[e], (to_right, to_left)[e]) for e in range(2)]

    def landed(k, q):
        i, _, g = tensors[k // 3]
        part = k % 3
        if part < 2:
            return [rows(g, i, chips - 1, q, part * h2, h2), rows(g, i, 1, q, (1 - part) * h2, h2)]
        return [rows(g, i, 2, q, 0, h2), rows(g, i, 2, q, h2, h2)]

    def core_copy(j, piece, q):
        i, src, g = tensors[j]
        if piece == 6:
            dst = rows(g, i, 0, q, 0, tok)
            return remote(src.at[i], dst, core_s.at[j, 6], core_r.at[j, 6], mate)
        ref = landed(3 * j + piece // 2, q)[piece % 2]
        return remote(ref, ref, core_s.at[j, piece], core_r.at[j, piece], mate)

    def own_copy(j):
        i, src, g = tensors[j]
        return pltpu.make_async_copy(src.at[i], rows(g, i, 0, core, 0, tok), own_sem.at[j])

    def issue(k):
        for c in ring_copies(k):
            c.start()
        if k < n_gather and k % 3 == 0:
            core_copy(k // 3, 6, core).start()
            own_copy(k // 3).start()

    last = n_gather + 3

    def event(k):
        for c in ring_copies(k):
            c.wait_recv()
        if k < n_gather:
            for e in range(2):
                core_copy(k // 3, 2 * (k % 3) + e, core).start()
        if k == n_gather:
            for e, s in ((RIGHT, 1), (LEFT, 3)):
                lo = s * tok + e * h2
                rs_send[2, e] = (gsum[lo:lo + h2, :] + rs_recv[0, e].astype(F32)).astype(BF16)
        if k + 2 < last:
            issue(k + 2)

    def gathered(j):
        for piece in range(7):
            core_copy(j, piece, 1 - core).wait_recv()
        own_copy(j).wait()

    def project(j, n_tiles, dot, dst):
        i, _, g = tensors[j]
        bm = xbuf.shape[1]

        def load(t, slot):
            return pltpu.make_async_copy(g.at[i, pl.ds(pl.multiple_of(t * bm, bm), bm), :], xbuf.at[slot], in_sem.at[slot])

        load(0, 0).start()

        def step(t, carry):
            slot = lax.rem(t, 2)

            @pl.when(t + 1 < seq // bm)
            def _():
                load(t + 1, 1 - slot).start()

            load(t, slot).wait()

            def col(c, carry):
                cols = pl.ds(pl.multiple_of(c * 256, 256), 256)
                dst[pl.ds(pl.multiple_of(t * bm, bm), bm), cols] = dot(xbuf[slot], cols).astype(BF16)
                return carry

            return lax.fori_loop(0, n_tiles, col, carry)

        lax.fori_loop(0, seq // bm, step, 0)

    def project_x(j):
        project(j, wide // 256, lambda a, cols: jnp.dot(a, wcat[:, cols], preferred_element_type=F32), nat)

    def project_y(j):
        project(j, qw // 256, lambda a, cols: lax.dot_general(a, wo[cols, :], NT, preferred_element_type=F32), donat)

    bq = CORES * tok
    row_id = lax.broadcasted_iota(jnp.int32, (bq, bq), 0)
    col_id = lax.broadcasted_iota(jnp.int32, (bq, bq), 1)

    def attention(events):
        dk_acc[...] = jnp.zeros_like(dk_acc)
        dv_acc[...] = jnp.zeros_like(dv_acc)

        def head(h, carry):
            lanes = pl.ds(pl.multiple_of(h * hd, hd), hd)
            for i in range(seq // bq):
                rs = slice(i * bq, (i + 1) * bq)
                n_k = (i + 1) * bq
                q = nat[rs, lanes]
                do = donat[rs, lanes]
                k = nat[:n_k, qw:qw + hd]
                v = nat[:n_k, qw + hd:]
                s = lax.dot_general(q, k, NT, preferred_element_type=F32)
                diag = jnp.where(row_id >= col_id, s[:, i * bq:], -jnp.inf)
                s = diag if i == 0 else jnp.concatenate([s[:, :i * bq], diag], axis=1)
                m = jnp.max(s, axis=1, keepdims=True)
                p = jnp.exp((s - m) * scale)
                p = p * (1.0 / jnp.sum(p, axis=1, keepdims=True))
                pb = p.astype(BF16)
                o = jnp.dot(pb, v, preferred_element_type=F32).astype(BF16)
                onat[rs, lanes] = o
                dp = lax.dot_general(do, v, NT, preferred_element_type=F32)
                dd = jnp.sum(do.astype(F32) * o.astype(F32), axis=1, keepdims=True)
                ds = (p * (dp - dd)).astype(BF16)
                dnat[rs, lanes] = (jnp.dot(ds, k, preferred_element_type=F32) * scale).astype(BF16)
                dk_acc[:n_k, :] += lax.dot_general(ds, q, TN, preferred_element_type=F32)
                dv_acc[:n_k, :] += lax.dot_general(pb, do, TN, preferred_element_type=F32)
            for at, ev in events:
                @pl.when(h == at)
                def _(ev=ev):
                    event(ev)
            return carry

        lax.fori_loop(0, heads, head, 0)
        dnat[:, qw:qw + hd] = (dk_acc[...] * scale).astype(BF16)
        dnat[:, qw + hd:] = dv_acc[...].astype(BF16)

    def out_copies(i):
        return (pltpu.make_async_copy(dnat, dqkv_out.at[i], out_sem.at[0]),
                pltpu.make_async_copy(onat, o_out.at[i], out_sem.at[1]))

    n_mate = mate_stage.shape[0]
    bn = d // n_mate

    def mate_copy(i, c):
        return remote(mate_stage.at[c], mate_recv.at[i, c], mate_s.at[i, c], mate_r.at[i, c], mate)

    def pick(q):
        for s in range(chips):
            lhs[s * tok:(s + 1) * tok, :] = dnat[pl.ds(pl.multiple_of(block(s, q), tok), tok), :]

    def dx_share(i):
        pick(1 - core)
        for c in range(n_mate):
            if i > 0:
                mate_copy(i - 1, c).wait_send()

            def tile(t, carry, c=c):
                w = wcat[pl.ds(pl.multiple_of(c * bn + t * 256, 256), 256), :]
                cols = pl.ds(pl.multiple_of(t * 256, 256), 256)
                mate_stage[c, :, cols] = lax.dot_general(lhs[...], w, NT, preferred_element_type=F32).astype(BF16)
                return carry

            lax.fori_loop(0, bn // 256, tile, 0)
            mate_copy(i, c).start()
        pick(core)
        for c in range(n_mate):
            mate_copy(i, c).wait_recv()

            def tile(t, carry, c=c):
                cols = pl.ds(pl.multiple_of(c * bn + t * 256, 256), 256)
                got = mate_recv[i, c, :, pl.ds(pl.multiple_of(t * 256, 256), 256)]
                gsum[:, cols] = lax.dot_general(lhs[...], wcat[cols, :], NT, preferred_element_type=F32) + got.astype(F32)
                return carry

            lax.fori_loop(0, bn // 256, tile, 0)

    def half(s, e):
        return gsum[s * tok + e * h2:s * tok + (e + 1) * h2, :]

    loads = [pltpu.make_async_copy(wcat_in, wcat, w_sem.at[0]), pltpu.make_async_copy(wo_in, wo, w_sem.at[1])]
    issue(0)
    issue(1)
    for c in loads:
        c.start()
    for k in range(3):
        event(k)
    for c in loads:
        c.wait()
    gathered(0)
    project_x(0)
    for k in range(3, 6):
        event(k)
    gathered(1)
    project_y(1)
    attention(((0, 6), (3, 7)))
    for c in out_copies(0):
        c.start()
    dx_share(0)
    for item, e, s, part in ((0, 0, 2, 0), (0, 1, 2, 1), (1, 0, 1, 1), (1, 1, 3, 0)):
        rs_send[item, e] = half(s, part).astype(BF16)
    dx_buf[...] = gsum[:tok, :]
    event(8)
    gathered(2)
    project_x(2)
    for k in range(9, 12):
        event(k)
    gathered(3)
    project_y(3)
    for c in out_copies(0):
        c.wait()
    attention(((0, 12), (3, 13)))
    for c in out_copies(1):
        c.start()
    dx_share(1)
    for item, (s, part) in enumerate(((2, 0), (2, 1), (1, 1), (3, 0))):
        snd_buf[item] = half(s, part).astype(BF16)
    outs = [pltpu.make_async_copy(snd_buf, snd_out, out_sem.at[2])]
    for item, (s, part) in enumerate(((1, 0), (3, 1), (0, 0), (0, 1))):
        lo = s * tok + part * h2
        outs.append(pltpu.make_async_copy(gsum.at[pl.ds(lo, h2), :], keep_out.at[item], out_sem.at[3 + item]))
    for c in outs:
        c.start()
    event(14)
    for c in ring_copies(n_gather):
        c.wait_send()
    lo = dx_buf[:h2, :] + rs_recv[2, RIGHT].astype(F32) + rs_recv[1, LEFT].astype(F32)
    hi = dx_buf[h2:, :] + rs_recv[1, RIGHT].astype(F32) + rs_recv[2, LEFT].astype(F32)
    rs_send[0, 0] = lo.astype(BF16)
    rs_send[0, 1] = hi.astype(BF16)
    fin = pltpu.make_async_copy(rs_send.at[0], dx_out, out_sem.at[7])
    fin.start()
    for k in range(last):
        if k != n_gather:
            for c in ring_copies(k):
                c.wait_send()
    for j in range(len(tensors)):
        for piece in range(7):
            core_copy(j, piece, core).wait_send()
    for c in range(n_mate):
        mate_copy(1, c).wait_send()
    for c in out_copies(1):
        c.wait()
    for c in outs:
        c.wait()
    fin.wait()


def fused(x, y, wcat, wo, chips, heads, hd):
    micro_n, tok, d = x.shape
    h2 = tok // 2
    seq = chips * CORES * tok
    qw, wide = heads * hd, (heads + 2) * hd
    half = chips * tok
    n_mate = 4
    any_spec = pl.BlockSpec(memory_space=pl.ANY)
    items = 6 * micro_n + 3
    dma = pltpu.SemaphoreType.DMA
    return pl.pallas_call(
        functools.partial(fused_kernel, chips, heads, hd),
        out_shape=(jax.ShapeDtypeStruct((micro_n, seq, d), BF16), jax.ShapeDtypeStruct((micro_n, seq, d), BF16),
                   jax.ShapeDtypeStruct((micro_n, seq, wide), BF16), jax.ShapeDtypeStruct((micro_n, seq, qw), BF16),
                   jax.ShapeDtypeStruct((2, h2, d), BF16), jax.ShapeDtypeStruct((4, h2, d), BF16),
                   jax.ShapeDtypeStruct((4, h2, d), F32)),
        in_specs=[any_spec] * 4,
        out_specs=(any_spec,) * 7,
        scratch_shapes=[
            pltpu.VMEM((d, wide), BF16), pltpu.VMEM((qw, d), BF16),
            pltpu.VMEM((seq, wide), BF16), pltpu.VMEM((seq, qw), BF16),
            pltpu.VMEM((seq, wide), BF16), pltpu.VMEM((seq, qw), BF16),
            pltpu.VMEM((seq, hd), F32), pltpu.VMEM((seq, hd), F32),
            pltpu.VMEM((2, 256, d), BF16), pltpu.VMEM((half, wide), BF16), pltpu.VMEM((half, d), F32),
            pltpu.VMEM((n_mate, half, d // n_mate), BF16), pltpu.VMEM((micro_n, n_mate, half, d // n_mate), BF16),
            pltpu.VMEM((3, 2, h2, d), BF16), pltpu.VMEM((3, 2, h2, d), BF16),
            pltpu.VMEM((tok, d), F32), pltpu.VMEM((4, h2, d), BF16),
            dma((items, 2)), dma((items, 2)), dma((2 * micro_n, 7)), dma((2 * micro_n, 7)),
            dma((micro_n, n_mate)), dma((micro_n, n_mate)), dma((2 * micro_n,)), dma((2,)), dma((2,)), dma((8,))],
        compiler_params=pltpu.CompilerParams(collective_id=0, has_side_effects=True,
                                             vmem_limit_bytes=67043328),
        cost_estimate=pl.CostEstimate(flops=10 ** 11, bytes_accessed=2 ** 27, transcendentals=0),
        name="fused",
    )(x, y, wcat, wo)


def wgrad_x_kernel(heads, hd, x, g, dwq, dwkv):
    out = lax.dot_general(x[0], g[0], TN, preferred_element_type=F32)
    for i in range(1, x.shape[0]):
        out += lax.dot_general(x[i], g[i], TN, preferred_element_type=F32)
    for h in range(heads):
        dwq[:, h, :] = out[:, h * hd:(h + 1) * hd]
    dwkv[...] = out[:, heads * hd:]


def wgrad_x(x, g, heads, hd):
    micro_n, seq, d = x.shape
    wide = g.shape[2]
    tile = 256
    return pl.pallas_call(
        functools.partial(wgrad_x_kernel, heads, hd),
        grid=(d // tile,),
        out_shape=(jax.ShapeDtypeStruct((d, heads, hd), F32), jax.ShapeDtypeStruct((d, 2 * hd), F32)),
        in_specs=[pl.BlockSpec((micro_n, seq, tile), lambda i: (0, 0, i)),
                  pl.BlockSpec((micro_n, seq, wide), lambda i: (0, 0, 0))],
        out_specs=(pl.BlockSpec((tile, heads, hd), lambda i: (i, 0, 0)), pl.BlockSpec((tile, 2 * hd), lambda i: (i, 0))),
        compiler_params=pltpu.CompilerParams(vmem_limit_bytes=32 * 2 ** 20),
        cost_estimate=pl.CostEstimate(flops=2 * micro_n * seq * d * wide, bytes_accessed=2 ** 25, transcendentals=0),
        name="wgrad_x",
    )(x, g)


def wgrad_o_kernel(o, y, dwo):
    out = lax.dot_general(o[0], y[0], TN, preferred_element_type=F32)
    for i in range(1, o.shape[0]):
        out += lax.dot_general(o[i], y[i], TN, preferred_element_type=F32)
    dwo[...] = out


def wgrad_o(o, y):
    micro_n, seq, d = y.shape
    qw = o.shape[2]
    tile = 512
    return pl.pallas_call(
        wgrad_o_kernel,
        grid=(d // tile,),
        out_shape=jax.ShapeDtypeStruct((qw, d), F32),
        in_specs=[pl.BlockSpec((micro_n, seq, qw), lambda i: (0, 0, 0)),
                  pl.BlockSpec((micro_n, seq, tile), lambda i: (0, 0, i))],
        out_specs=pl.BlockSpec((qw, tile), lambda i: (0, i)),
        compiler_params=pltpu.CompilerParams(vmem_limit_bytes=32 * 2 ** 20),
        cost_estimate=pl.CostEstimate(flops=2 * micro_n * seq * d * qw, bytes_accessed=2 ** 25, transcendentals=0),
        name="wgrad_o",
    )(o, y)


def solution(mesh):
    n = mesh.shape["model"]
    chips = n // CORES
    right = [(i, (i + CORES) % n) for i in range(n)]
    left = [(i, (i - CORES) % n) for i in range(n)]
    swap = [(i, i ^ 1) for i in range(n)]
    pair = [(i, i ^ 2) for i in range(n)]

    def send(a, pairs):
        return lax.ppermute(a, "model", pairs)

    def ring_tail(snd, keep):
        in_r0 = send(snd[0], right)
        in_l1 = send(snd[1], left)
        b1 = send(snd[2], right)
        c0 = send(snd[3], left)
        b0 = send((keep[0] + in_r0.astype(F32)).astype(BF16), right)
        c1 = send((keep[1] + in_l1.astype(F32)).astype(BF16), left)
        lo = keep[2] + b0.astype(F32) + c0.astype(F32)
        hi = keep[3] + b1.astype(F32) + c1.astype(F32)
        return jnp.concatenate([lo, hi]).astype(BF16)

    def device_grads(x_loc, dy_loc, w_q, w_k, w_v, w_o):
        micro_n, tok, d = x_loc.shape
        heads, hd = w_q.shape[1], w_q.shape[2]
        qw = heads * hd
        idx = lax.axis_index("model")
        chip, core = idx // CORES, idx % CORES
        kv = idx // (n // w_k.shape[1])
        wk = lax.dynamic_index_in_dim(w_k, kv, axis=1, keepdims=False)
        wv = lax.dynamic_index_in_dim(w_v, kv, axis=1, keepdims=False)
        wcat = jnp.concatenate([w_q.reshape(d, qw), wk, wv], axis=1)
        xg, yg, g, o, dx1, snd, keep = fused(x_loc, dy_loc, wcat, w_o.reshape(qw, d), chips, heads, hd)
        dwq, dwkv = wgrad_x(xg, g, heads, hd)
        dwo = wgrad_o(o, yg)
        dx2 = ring_tail(snd, keep)
        quarter = d // (n // w_k.shape[1])
        kv4 = dwkv.reshape(2, 2, quarter, 2 * hd)
        give = lax.dynamic_index_in_dim(kv4, 1 - core, axis=1, keepdims=False)
        part = lax.dynamic_index_in_dim(kv4, core, axis=1, keepdims=False) + send(give, swap)
        give = lax.dynamic_index_in_dim(part, 1 - chip % 2, axis=0, keepdims=False)
        own = lax.dynamic_index_in_dim(part, chip % 2, axis=0, keepdims=False) + send(give, pair)
        return (jnp.stack([dx1.reshape(tok, d), dx2]), dwq, own[:, :hd], own[:, hd:], dwo.reshape(heads, hd, d))

    return jax.shard_map(
        device_grads, mesh=mesh,
        in_specs=(P("data", "model", None), P("data", "model", None), P(None, "model", None),
                  P(None, None, None), P(None, None, None), P("model", None, None)),
        out_specs=(P("data", "model", None), P("data", "model", None), P(("data", "model"), None),
                   P(("data", "model"), None), P(("data", "model"), None, None)),
        check_vma=False)
```

```python
import functools

import jax
import jax.numpy as jnp
from jax import lax
from jax.experimental import pallas as pl
from jax.experimental.pallas import tpu as pltpu
from jax.sharding import PartitionSpec as P

F32 = jnp.float32
BF16 = jnp.bfloat16
NT = (((1,), (1,)), ((), ()))
TN = (((0,), (0,)), ((), ()))
CORES = 2
RIGHT, LEFT = 0, 1
MESH = pl.DeviceIdType.MESH


def fused_kernel(chips, heads, hd, kv_heads, x_in, y_in, wq_in, wk_in, wv_in, wo_in, l0_in, r1_in,
                 xg, yg, dq_out, o_out, kv_out, dx_out, o0_out, o1_out, b1_out, c0_out, r0_out, l1_out, own_out, dwq_out, dwo_out,
                 wcat, wo, nat, donat, dnat, onat, dk_acc, dv_acc, xbuf, lhs, gsum,
                 mate_stage, mate_recv, rs_send, rs_recv, dx_buf, snd_buf, kvp, kv_in, kv_all, tbuf, qbuf, obuf,
                 ring_s, ring_r, core_s, core_r, mate_s, mate_r, kv_s, kv_r, own_sem, w_sem, in_sem, out_sem, tile_sem):
    micro_n, tok, d = x_in.shape
    h2 = tok // 2
    n = chips * CORES
    qw = heads * hd
    wide = qw + 2 * hd
    seq = n * tok
    me = lax.axis_index("model")
    chip, core = me // CORES, lax.rem(me, CORES)
    to_right, to_left = lax.rem(me + CORES, n), lax.rem(me + n - CORES, n)
    mate = chip * CORES + 1 - core
    spot = lax.rem(chip, 2)
    pair = me + CORES - 2 * CORES * spot
    scale = hd ** -0.5

    def chip_at(s):
        return lax.rem(chip + s, chips)

    def block(s, q):
        return (chip_at(s) * CORES + q) * tok

    def rows(ref, i, s, q, off, size):
        return ref.at[i, pl.ds(pl.multiple_of(block(s, q) + off, h2), size), :]

    def remote(src, dst, s_sem, r_sem, dev):
        return pltpu.make_async_remote_copy(src_ref=src, dst_ref=dst, send_sem=s_sem, recv_sem=r_sem,
                                            device_id={"model": dev}, device_id_type=MESH)

    barrier = pltpu.get_barrier_semaphore()
    for dev in (to_right, to_left, mate):
        pl.semaphore_signal(barrier, inc=1, device_id={"model": dev}, device_id_type=MESH)
    pl.semaphore_wait(barrier, 3)

    tensors = []
    for i in range(micro_n):
        tensors += [(i, x_in, xg), (i, y_in, yg)]
    n_gather = 3 * len(tensors)

    def ring_copies(k):
        sems = [(ring_s.at[k, e], ring_r.at[k, e]) for e in range(2)]
        if k < n_gather:
            i, src, g = tensors[k // 3]
            part = k % 3
            if part < 2:
                offs = (part * h2, (1 - part) * h2)
                srcs = [src.at[i, pl.ds(off, h2), :] for off in offs]
                dsts = [rows(g, i, 0, core, off, h2) for off in offs]
            else:
                srcs = dsts = [rows(g, i, chips - 1, core, 0, h2), rows(g, i, 1, core, h2, h2)]
                if k == 2:
                    srcs = [l0_in, r1_in]
        else:
            srcs = [rs_send.at[k - n_gather, e] for e in range(2)]
            dsts = [rs_recv.at[k - n_gather, e] for e in range(2)]
        return [remote(srcs[e], dsts[e], *sems[e], (to_right, to_left)[e]) for e in range(2)]

    def landed(k, q):
        i, _, g = tensors[k // 3]
        part = k % 3
        if part < 2:
            return [rows(g, i, chips - 1, q, part * h2, h2), rows(g, i, 1, q, (1 - part) * h2, h2)]
        return [rows(g, i, 2, q, 0, h2), rows(g, i, 2, q, h2, h2)]

    def core_copy(j, piece, q):
        i, src, g = tensors[j]
        if piece == 6:
            dst = rows(g, i, 0, q, 0, tok)
            return remote(src.at[i], dst, core_s.at[j, 6], core_r.at[j, 6], mate)
        ref = landed(3 * j + piece // 2, q)[piece % 2]
        return remote((l0_in, r1_in)[piece] if j == 0 and piece < 2 else ref, ref, core_s.at[j, piece], core_r.at[j, piece], mate)

    local_copies = []
    for j, (i, src, g) in enumerate(tensors):
        mid = xbuf.at[j // 2, pl.ds(j % 2 * tok, tok), :]
        local_copies.append((src.at[i], mid, rows(g, i, 0, core, 0, tok)))
    for e, src in enumerate((l0_in, r1_in)):
        local_copies.append((src, rs_send.at[0, e], landed(0, core)[e]))
    to_vmem = [pltpu.make_async_copy(a, b, own_sem.at[0, j]) for j, (a, b, c) in enumerate(local_copies)]
    to_hbm = [pltpu.make_async_copy(b, c, own_sem.at[1, j]) for j, (a, b, c) in enumerate(local_copies)]

    def issue(k):
        for c in ring_copies(k):
            c.start()
        if k < n_gather and k % 3 == 0:
            core_copy(k // 3, 6, core).start()

    last = n_gather + 3

    def event(k):
        if k > 0:
            for c in ring_copies(k):
                c.wait_recv()
        if k < n_gather:
            for e in range(2):
                core_copy(k // 3, 2 * (k % 3) + e, core).start()
        if k == n_gather:
            for e, s in ((RIGHT, 1), (LEFT, 3)):
                lo = s * tok + e * h2
                rs_send[2, e] = (gsum[lo:lo + h2, :] + rs_recv[0, e].astype(F32)).astype(BF16)
        if k + 2 < last:
            issue(k + 2)

    def gathered(j):
        for piece in range(7):
            core_copy(j, piece, 1 - core).wait_recv()

    def project(j, n_tiles, dot, dst):
        i, _, g = tensors[j]
        bm = xbuf.shape[1]

        def load(t, slot):
            return pltpu.make_async_copy(g.at[i, pl.ds(pl.multiple_of(t * bm, bm), bm), :], xbuf.at[slot], in_sem.at[slot])

        load(0, 0).start()

        def step(t, carry):
            slot = lax.rem(t, 2)

            @pl.when(t + 1 < seq // bm)
            def _():
                load(t + 1, 1 - slot).start()

            load(t, slot).wait()

            def col(c, carry):
                cols = pl.ds(pl.multiple_of(c * 256, 256), 256)
                dst[pl.ds(pl.multiple_of(t * bm, bm), bm), cols] = dot(xbuf[slot], cols).astype(BF16)
                return carry

            return lax.fori_loop(0, n_tiles, col, carry)

        lax.fori_loop(0, seq // bm, step, 0)

    def project_x(j):
        project(j, wide // 256, lambda a, cols: jnp.dot(a, wcat[:, cols], preferred_element_type=F32), nat)

    def project_y(j):
        project(j, qw // 256, lambda a, cols: lax.dot_general(a, wo[cols, :], NT, preferred_element_type=F32), donat)

    bq = CORES * tok
    row_id = lax.broadcasted_iota(jnp.int32, (bq, bq), 0)
    col_id = lax.broadcasted_iota(jnp.int32, (bq, bq), 1)

    def attention(events):
        dk_acc[...] = jnp.zeros_like(dk_acc)
        dv_acc[...] = jnp.zeros_like(dv_acc)

        def head(h, carry):
            lanes = pl.ds(pl.multiple_of(h * hd, hd), hd)
            for i in range(seq // bq):
                rs = slice(i * bq, (i + 1) * bq)
                n_k = (i + 1) * bq
                q = nat[rs, lanes]
                do = donat[rs, lanes]
                k = nat[:n_k, qw:qw + hd]
                v = nat[:n_k, qw + hd:]
                s = lax.dot_general(q, k, NT, preferred_element_type=F32)
                diag = jnp.where(row_id >= col_id, s[:, i * bq:], -jnp.inf)
                s = diag if i == 0 else jnp.concatenate([s[:, :i * bq], diag], axis=1)
                m = jnp.max(s, axis=1, keepdims=True)
                p = jnp.exp((s - m) * scale)
                p = p * (1.0 / jnp.sum(p, axis=1, keepdims=True))
                pb = p.astype(BF16)
                o = jnp.dot(pb, v, preferred_element_type=F32).astype(BF16)
                onat[rs, lanes] = o
                dp = lax.dot_general(do, v, NT, preferred_element_type=F32)
                dd = jnp.sum(do.astype(F32) * o.astype(F32), axis=1, keepdims=True)
                ds = (p * (dp - dd)).astype(BF16)
                dnat[rs, lanes] = (jnp.dot(ds, k, preferred_element_type=F32) * scale).astype(BF16)
                dk_acc[:n_k, :] += lax.dot_general(ds, q, TN, preferred_element_type=F32)
                dv_acc[:n_k, :] += lax.dot_general(pb, do, TN, preferred_element_type=F32)
            for at, ev in events:
                @pl.when(h == at)
                def _(ev=ev):
                    event(ev)
            return carry

        lax.fori_loop(0, heads, head, 0)
        dnat[:, qw:qw + hd] = (dk_acc[...] * scale).astype(BF16)
        dnat[:, qw + hd:] = dv_acc[...].astype(BF16)

    def out_copies():
        return (pltpu.make_async_copy(dnat.at[:, pl.ds(0, qw)], dq_out, out_sem.at[0]),
                pltpu.make_async_copy(onat, o_out, out_sem.at[1]))

    hs = seq // 2

    def kv_copy(i, what):
        mine = kv_all.at[i, spot, pl.ds(pl.multiple_of(core * hs, hs), hs), :]
        theirs = kv_all.at[i, 1 - spot, pl.ds(pl.multiple_of(core * hs, hs), hs), :]
        give = kvp.at[pl.ds(pl.multiple_of((1 - core) * hs, hs), hs), :]
        src, dst, dev = ((give, kv_in.at[i], mate), (mine, mine, pair), (mine, mine, mate), (theirs, theirs, mate))[what]
        return remote(src, dst, kv_s.at[i, what], kv_r.at[i, what], dev)

    def kv_start(i):
        if i > 0:
            kv_copy(i - 1, 0).wait_send()
        kvp[:, :hd] = dk_acc[...] * scale
        kvp[:, hd:] = dv_acc[...]
        kv_copy(i, 0).start()

    def kv_sum(i):
        kv_copy(i, 0).wait_recv()
        at = pl.ds(pl.multiple_of(core * hs, hs), hs)
        kv_all[i, spot, at, :] = (kvp[at, :] + kv_in[i]).astype(BF16)
        kv_copy(i, 1).start()
        kv_copy(i, 2).start()

    def kv_forward(i):
        kv_copy(i, 1).wait_recv()
        kv_copy(i, 3).start()

    def kv_finish(i):
        kv_copy(i, 2).wait_recv()
        kv_copy(i, 3).wait_recv()

    n_mate = mate_stage.shape[0]
    bn = d // n_mate

    def mate_copy(i, c):
        return remote(mate_stage.at[c], mate_recv.at[i, c], mate_s.at[i, c], mate_r.at[i, c], mate)

    def pick(q):
        for s in range(chips):
            lhs[s * tok:(s + 1) * tok, :] = dnat[pl.ds(pl.multiple_of(block(s, q), tok), tok), :]

    def dx_share(i):
        pick(1 - core)
        for c in range(n_mate):
            if i > 0:
                mate_copy(i - 1, c).wait_send()

            def tile(t, carry, c=c):
                w = wcat[pl.ds(pl.multiple_of(c * bn + t * 256, 256), 256), :]
                cols = pl.ds(pl.multiple_of(t * 256, 256), 256)
                mate_stage[c, :, cols] = lax.dot_general(lhs[...], w, NT, preferred_element_type=F32).astype(BF16)
                return carry

            lax.fori_loop(0, bn // 256, tile, 0)
            mate_copy(i, c).start()
        kv_sum(i)
        pick(core)
        for c in range(n_mate):
            mate_copy(i, c).wait_recv()

            def tile(t, carry, c=c):
                cols = pl.ds(pl.multiple_of(c * bn + t * 256, 256), 256)
                got = mate_recv[i, c, :, pl.ds(pl.multiple_of(t * 256, 256), 256)]
                gsum[:, cols] = lax.dot_general(lhs[...], wcat[cols, :], NT, preferred_element_type=F32) + got.astype(F32)
                return carry

            lax.fori_loop(0, bn // 256, tile, 0)

    def wgrad(g, i, buf, put, dot):
        bt = tbuf.shape[2]
        tiles = d // bt

        def cols(t):
            return pl.ds(pl.multiple_of(t * bt, bt), bt)

        def load(t, slot):
            return pltpu.make_async_copy(g.at[i, :, cols(t)], tbuf.at[slot], tile_sem.at[0, slot])

        def save(t, slot):
            return pltpu.make_async_copy(buf.at[slot], put(cols(t)), tile_sem.at[1, slot])

        deep = tbuf.shape[0]
        for t in range(deep - 1):
            load(t, t).start()

        def step(t, carry):
            slot = lax.rem(t, deep)

            @pl.when(t + deep - 1 < tiles)
            def _():
                load(t + deep - 1, lax.rem(t + deep - 1, deep)).start()

            load(t, slot).wait()

            @pl.when(t >= deep)
            def _():
                save(t - deep, slot).wait()

            buf[slot] = dot(tbuf[slot])
            save(t, slot).start()
            return carry

        lax.fori_loop(0, tiles, step, 0)
        for t in range(tiles - deep, tiles):
            save(t, t % deep).wait()

    def half(s, e):
        return gsum[s * tok + e * h2:s * tok + (e + 1) * h2, :]

    kv_cols = pl.ds(pl.multiple_of(me // (n // kv_heads) * hd, hd), hd)
    loads = [pltpu.make_async_copy(wq_in, wcat.at[:, pl.ds(0, qw)], w_sem.at[0]),
             pltpu.make_async_copy(wk_in.at[:, kv_cols], wcat.at[:, pl.ds(qw, hd)], w_sem.at[1]),
             pltpu.make_async_copy(wv_in.at[:, kv_cols], wcat.at[:, pl.ds(qw + hd, hd)], w_sem.at[2]),
             pltpu.make_async_copy(wo_in, wo, w_sem.at[3])]
    issue(1)
    core_copy(0, 6, core).start()
    for c in to_vmem:
        c.start()
    for c in loads:
        c.start()
    event(0)
    for c, w in zip(to_vmem, to_hbm):
        c.wait()
        w.start()
    for k in range(1, 3):
        event(k)
    for c in to_hbm:
        c.wait()
    for c in loads:
        c.wait()
    gathered(0)
    project_x(0)
    for k in range(3, 6):
        event(k)
    gathered(1)
    project_y(1)
    attention(((0, 6), (3, 7)))
    kv_start(0)
    dx_share(0)
    for item, e, s, part in ((0, 0, 2, 0), (0, 1, 2, 1), (1, 0, 1, 1), (1, 1, 3, 0)):
        rs_send[item, e] = half(s, part).astype(BF16)
    dx_buf[...] = gsum[:tok, :]
    event(8)
    gathered(2)
    project_x(2)
    event(9)
    kv_forward(0)
    wgrad(xg, 0, qbuf, lambda cols: dwq_out.at[cols, :],
          lambda a: lax.dot_general(a, dnat[:, :qw], TN, preferred_element_type=F32))
    event(10)
    wgrad(yg, 0, obuf, lambda cols: dwo_out.at[:, cols],
          lambda a: lax.dot_general(onat[...], a, TN, preferred_element_type=F32))
    event(11)
    gathered(3)
    project_y(3)
    attention(((0, 12), (3, 13)))
    kv_start(1)
    for c in out_copies():
        c.start()
    dx_share(1)
    outs = []
    for item, (s, part, out) in enumerate(((2, 0, o0_out), (2, 1, o1_out), (1, 1, b1_out), (3, 0, c0_out))):
        snd_buf[item] = half(s, part).astype(BF16)
        outs.append(pltpu.make_async_copy(snd_buf.at[item], out, out_sem.at[2 + item]))
        outs[-1].start()
    for item, (lo, size, out) in enumerate(((tok, h2, r0_out), (3 * tok + h2, h2, l1_out), (0, tok, own_out))):
        outs.append(pltpu.make_async_copy(gsum.at[pl.ds(lo, size), :], out, out_sem.at[6 + item]))
        outs[-1].start()
    event(14)
    kv_forward(1)
    for c in ring_copies(n_gather):
        c.wait_send()
    lo = dx_buf[:h2, :] + rs_recv[2, RIGHT].astype(F32) + rs_recv[1, LEFT].astype(F32)
    hi = dx_buf[h2:, :] + rs_recv[1, RIGHT].astype(F32) + rs_recv[2, LEFT].astype(F32)
    rs_send[0, 0] = lo.astype(BF16)
    rs_send[0, 1] = hi.astype(BF16)
    fin = pltpu.make_async_copy(rs_send.at[0], dx_out, out_sem.at[9])
    fin.start()
    for i in range(micro_n):
        kv_finish(i)
    kv_save = pltpu.make_async_copy(kv_all, kv_out, out_sem.at[10])
    kv_save.start()
    for k in range(1, last):
        if k != n_gather:
            for c in ring_copies(k):
                c.wait_send()
    for j in range(len(tensors)):
        for piece in range(7):
            core_copy(j, piece, core).wait_send()
    for c in range(n_mate):
        mate_copy(1, c).wait_send()
    kv_copy(1, 0).wait_send()
    for i in range(micro_n):
        for what in range(1, 4):
            kv_copy(i, what).wait_send()
    kv_save.wait()
    for c in out_copies():
        c.wait()
    for c in outs:
        c.wait()
    fin.wait()


def fused(x, y, wq, wk, wv, wo, l0, r1, chips, heads, hd):
    micro_n, tok, d = x.shape
    h2 = tok // 2
    seq = chips * CORES * tok
    qw, wide = heads * hd, (heads + 2) * hd
    half = chips * tok
    n_mate = 4
    any_spec = pl.BlockSpec(memory_space=pl.ANY)
    items = 6 * micro_n + 3
    dma = pltpu.SemaphoreType.DMA
    part16, part32 = jax.ShapeDtypeStruct((h2, d), BF16), jax.ShapeDtypeStruct((h2, d), F32)
    return pl.pallas_call(
        functools.partial(fused_kernel, chips, heads, hd, wk.shape[1] // hd),
        out_shape=(jax.ShapeDtypeStruct((micro_n, seq, d), BF16), jax.ShapeDtypeStruct((micro_n, seq, d), BF16),
                   jax.ShapeDtypeStruct((seq, qw), BF16), jax.ShapeDtypeStruct((seq, qw), BF16),
                   jax.ShapeDtypeStruct((micro_n, 2, seq, 2 * hd), BF16), jax.ShapeDtypeStruct((2, h2, d), BF16),
                   part16, part16, part16, part16, part32, part32, jax.ShapeDtypeStruct((tok, d), F32),
                   jax.ShapeDtypeStruct((d, qw), F32), jax.ShapeDtypeStruct((qw, d), F32)),
        in_specs=[any_spec] * 8,
        out_specs=(any_spec,) * 15,
        scratch_shapes=[
            pltpu.VMEM((d, wide), BF16), pltpu.VMEM((qw, d), BF16),
            pltpu.VMEM((seq, wide), BF16), pltpu.VMEM((seq, qw), BF16),
            pltpu.VMEM((seq, wide), BF16), pltpu.VMEM((seq, qw), BF16),
            pltpu.VMEM((seq, hd), F32), pltpu.VMEM((seq, hd), F32),
            pltpu.VMEM((2, 256, d), BF16), pltpu.VMEM((half, wide), BF16), pltpu.VMEM((half, d), F32),
            pltpu.VMEM((n_mate, half, d // n_mate), BF16), pltpu.VMEM((micro_n, n_mate, half, d // n_mate), BF16),
            pltpu.VMEM((3, 2, h2, d), BF16), pltpu.VMEM((3, 2, h2, d), BF16),
            pltpu.VMEM((tok, d), F32), pltpu.VMEM((4, h2, d), BF16),
            pltpu.VMEM((seq, 2 * hd), F32), pltpu.VMEM((micro_n, seq // 2, 2 * hd), F32),
            pltpu.VMEM((micro_n, 2, seq, 2 * hd), BF16),
            pltpu.VMEM((4, seq, 256), BF16), pltpu.VMEM((4, 256, qw), F32), pltpu.VMEM((4, qw, 256), F32),
            dma((items, 2)), dma((items, 2)), dma((2 * micro_n, 7)), dma((2 * micro_n, 7)),
            dma((micro_n, n_mate)), dma((micro_n, n_mate)), dma((micro_n, 4)), dma((micro_n, 4)),
            dma((2, 2 * micro_n + 2)), dma((4,)), dma((2,)), dma((11,)), dma((2, 4))],
        compiler_params=pltpu.CompilerParams(collective_id=0, has_side_effects=True,
                                             vmem_limit_bytes=67043328),
        cost_estimate=pl.CostEstimate(flops=10 ** 11, bytes_accessed=2 ** 27, transcendentals=0),
        name="fused",
    )(x, y, wq, wk, wv, wo, l0, r1)


def wgrad_x_kernel(heads, hd, x, g, prev, dwq):
    out = prev[...] + lax.dot_general(x[...], g[...], TN, preferred_element_type=F32)
    for h in range(heads):
        dwq[:, h, :] = out[:, h * hd:(h + 1) * hd]


def wgrad_x(x, g, prev, heads, hd):
    micro_n, seq, d = x.shape
    qw = g.shape[1]
    tile = 512
    return pl.pallas_call(
        functools.partial(wgrad_x_kernel, heads, hd),
        grid=(d // tile,),
        out_shape=jax.ShapeDtypeStruct((d, heads, hd), F32),
        in_specs=[pl.BlockSpec((None, seq, tile), lambda i: (micro_n - 1, 0, i)),
                  pl.BlockSpec((seq, qw), lambda i: (0, 0)),
                  pl.BlockSpec((tile, qw), lambda i: (i, 0))],
        out_specs=pl.BlockSpec((tile, heads, hd), lambda i: (i, 0, 0)),
        compiler_params=pltpu.CompilerParams(vmem_limit_bytes=62 * 2 ** 20),
        cost_estimate=pl.CostEstimate(flops=2 * seq * d * qw, bytes_accessed=2 ** 25, transcendentals=0),
        name="wgrad_x",
    )(x, g, prev)


def wgrad_kv_kernel(hd, _, x, kv, dwk, dwv):
    out = None
    for i in range(kv.shape[0]):
        for j in range(kv.shape[1]):
            term = lax.dot_general(x[i], kv[i, j], TN, preferred_element_type=F32)
            out = term if out is None else out + term
    dwk[...] = out[:, :hd]
    dwv[...] = out[:, hd:]


def wgrad_kv(x, kv, sub, group):
    micro_n, seq, d = x.shape
    hd = kv.shape[3] // 2
    tile = 256
    per = d // group // tile
    out = pl.BlockSpec((tile, hd), lambda i, at: (i, 0))
    return pl.pallas_call(
        functools.partial(wgrad_kv_kernel, hd),
        grid_spec=pltpu.PrefetchScalarGridSpec(
            num_scalar_prefetch=1, grid=(per,),
            in_specs=[pl.BlockSpec((micro_n, seq, tile), lambda i, at: (0, 0, at[0] * per + i)),
                      pl.BlockSpec(kv.shape, lambda i, at: (0, 0, 0, 0))],
            out_specs=(out, out)),
        out_shape=(jax.ShapeDtypeStruct((d // group, hd), F32),) * 2,
        compiler_params=pltpu.CompilerParams(vmem_limit_bytes=62 * 2 ** 20),
        cost_estimate=pl.CostEstimate(flops=8 * micro_n * seq * (d // group) * hd, bytes_accessed=2 ** 23,
                                      transcendentals=0),
        name="wgrad_kv",
    )(sub.reshape(1), x, kv)


def wgrad_o_kernel(o, y, prev, dwo):
    dwo[...] = prev[...] + lax.dot_general(o[...], y[...], TN, preferred_element_type=F32)


def wgrad_o(o, y, prev):
    micro_n, seq, d = y.shape
    qw = o.shape[1]
    tile = 1024
    out = pl.BlockSpec((qw, tile), lambda i: (0, i))
    return pl.pallas_call(
        wgrad_o_kernel,
        grid=(d // tile,),
        out_shape=jax.ShapeDtypeStruct((qw, d), F32),
        in_specs=[pl.BlockSpec((seq, qw), lambda i: (0, 0)),
                  pl.BlockSpec((None, seq, tile), lambda i: (micro_n - 1, 0, i)),
                  pl.BlockSpec((qw, tile), lambda i: (0, i))],
        out_specs=out,
        compiler_params=pltpu.CompilerParams(vmem_limit_bytes=62 * 2 ** 20),
        cost_estimate=pl.CostEstimate(flops=2 * seq * d * qw, bytes_accessed=2 ** 25, transcendentals=0),
        name="wgrad_o",
    )(o, y, prev)


def solution(mesh):
    n = mesh.shape["model"]
    chips = n // CORES
    right = [(i, (i + CORES) % n) for i in range(n)]
    left = [(i, (i - CORES) % n) for i in range(n)]

    def send(a, pairs):
        return lax.ppermute(a, "model", pairs)

    def device_grads(x_loc, dy_loc, w_q, w_k, w_v, w_o):
        micro_n, tok, d = x_loc.shape
        heads, hd = w_q.shape[1], w_q.shape[2]
        kv_heads = w_k.shape[1]
        group = n // kv_heads
        qw = heads * hd
        l0 = send(x_loc[0, :tok // 2], right)
        r1 = send(x_loc[0, tok // 2:], left)
        xg, yg, dq, o, kv, dx1, *tail = fused(
            x_loc, dy_loc, w_q.reshape(d, qw), w_k.reshape(d, kv_heads * hd), w_v.reshape(d, kv_heads * hd),
            w_o.reshape(qw, d), l0, r1, chips, heads, hd)
        o0, o1, b1, c0, r0, l1, own, dwq1, dwo1 = tail
        in_r0, in_l1 = send(o0, right), send(o1, left)
        b1, c0 = send(b1, right), send(c0, left)
        dwo = wgrad_o(o, yg, dwo1)
        in_r0, in_l1, dwo = lax.optimization_barrier((in_r0, in_l1, dwo))
        b0 = (r0 + in_r0.astype(F32)).astype(BF16)
        c1 = (l1 + in_l1.astype(F32)).astype(BF16)
        b0, c1, dq = lax.optimization_barrier((b0, c1, dq))
        b0, c1 = send(b0, right), send(c1, left)
        dwq = wgrad_x(xg, dq, dwq1, heads, hd)
        dwk, dwv = wgrad_kv(xg, kv, lax.axis_index("model") % group, group)
        from_left = jnp.concatenate([b0, b1]).astype(F32)
        from_right = jnp.concatenate([c0, c1]).astype(F32)
        dx2 = (own + from_left + from_right).astype(BF16)
        return (jnp.stack([dx1.reshape(tok, d), dx2]), dwq, dwk, dwv, dwo.reshape(heads, hd, d))

    return jax.shard_map(
        device_grads, mesh=mesh,
        in_specs=(P("data", "model", None), P("data", "model", None), P(None, "model", None),
                  P(None, None, None), P(None, None, None), P("model", None, None)),
        out_specs=(P("data", "model", None), P("data", "model", None), P(("data", "model"), None),
                   P(("data", "model"), None), P(("data", "model"), None, None)),
        check_vma=False)
```

```python
import functools

import jax
import jax.numpy as jnp
from jax import lax
from jax.experimental import pallas as pl
from jax.experimental.pallas import tpu as pltpu
from jax.sharding import PartitionSpec as P

F32 = jnp.float32
BF16 = jnp.bfloat16
NT = (((1,), (1,)), ((), ()))
TN = (((0,), (0,)), ((), ()))
CORES = 2
RIGHT, LEFT = 0, 1
MESH = pl.DeviceIdType.MESH


def fused_kernel(chips, heads, hd, kv_heads, x_in, y_in, wq_in, wk_in, wv_in, wo_in, l0_in, r1_in,
                 xg, yg, dq_out, o_out, kv_out, dx_out, o0_out, o1_out, b1_out, c0_out, r0_out, l1_out, own_out, dwq_out, dwo_out,
                 wcat, wo, nat, donat, dnat, onat, dk_acc, dv_acc, xbuf, lhs, gsum,
                 mate_stage, mate_recv, rs_send, rs_recv, dx_buf, snd_buf, kvp, kv_in, kv_all, tbuf, qbuf, obuf,
                 ring_s, ring_r, core_s, core_r, mate_s, mate_r, kv_s, kv_r, own_sem, w_sem, in_sem, out_sem, tile_sem):
    micro_n, tok, d = x_in.shape
    h2 = tok // 2
    n = chips * CORES
    qw = heads * hd
    wide = qw + 2 * hd
    seq = n * tok
    me = lax.axis_index("model")
    chip, core = me // CORES, lax.rem(me, CORES)
    to_right, to_left = lax.rem(me + CORES, n), lax.rem(me + n - CORES, n)
    mate = chip * CORES + 1 - core
    spot = lax.rem(chip, 2)
    pair = me + CORES - 2 * CORES * spot
    scale = hd ** -0.5

    def chip_at(s):
        return lax.rem(chip + s, chips)

    def block(s, q):
        return (chip_at(s) * CORES + q) * tok

    def rows(ref, i, s, q, off, size):
        return ref.at[i, pl.ds(pl.multiple_of(block(s, q) + off, h2), size), :]

    def remote(src, dst, s_sem, r_sem, dev):
        return pltpu.make_async_remote_copy(src_ref=src, dst_ref=dst, send_sem=s_sem, recv_sem=r_sem,
                                            device_id={"model": dev}, device_id_type=MESH)

    barrier = pltpu.get_barrier_semaphore()
    for dev in (to_right, to_left, mate):
        pl.semaphore_signal(barrier, inc=1, device_id={"model": dev}, device_id_type=MESH)
    pl.semaphore_wait(barrier, 3)

    tensors = []
    for i in range(micro_n):
        tensors += [(i, x_in, xg), (i, y_in, yg)]
    n_gather = 3 * len(tensors)

    def ring_copies(k):
        sems = [(ring_s.at[k, e], ring_r.at[k, e]) for e in range(2)]
        if k < n_gather:
            i, src, g = tensors[k // 3]
            part = k % 3
            if part < 2:
                offs = (part * h2, (1 - part) * h2)
                srcs = [src.at[i, pl.ds(off, h2), :] for off in offs]
                dsts = [rows(g, i, 0, core, off, h2) for off in offs]
            else:
                srcs = dsts = [rows(g, i, chips - 1, core, 0, h2), rows(g, i, 1, core, h2, h2)]
                if k == 2:
                    srcs = [l0_in, r1_in]
        else:
            srcs = [rs_send.at[k - n_gather, e] for e in range(2)]
            dsts = [rs_recv.at[k - n_gather, e] for e in range(2)]
        return [remote(srcs[e], dsts[e], *sems[e], (to_right, to_left)[e]) for e in range(2)]

    def landed(k, q):
        i, _, g = tensors[k // 3]
        part = k % 3
        if part < 2:
            return [rows(g, i, chips - 1, q, part * h2, h2), rows(g, i, 1, q, (1 - part) * h2, h2)]
        return [rows(g, i, 2, q, 0, h2), rows(g, i, 2, q, h2, h2)]

    def core_copy(j, piece, q):
        i, src, g = tensors[j]
        if piece == 6:
            dst = rows(g, i, 0, q, 0, tok)
            return remote(src.at[i], dst, core_s.at[j, 6], core_r.at[j, 6], mate)
        ref = landed(3 * j + piece // 2, q)[piece % 2]
        return remote((l0_in, r1_in)[piece] if j == 0 and piece < 2 else ref, ref, core_s.at[j, piece], core_r.at[j, piece], mate)

    local_copies = []
    for j, (i, src, g) in enumerate(tensors):
        mid = xbuf.at[j // 2, pl.ds(j % 2 * tok, tok), :]
        local_copies.append((src.at[i], mid, rows(g, i, 0, core, 0, tok)))
    for e, src in enumerate((l0_in, r1_in)):
        local_copies.append((src, rs_send.at[0, e], landed(0, core)[e]))
    to_vmem = [pltpu.make_async_copy(a, b, own_sem.at[0, j]) for j, (a, b, c) in enumerate(local_copies)]
    to_hbm = [pltpu.make_async_copy(b, c, own_sem.at[1, j]) for j, (a, b, c) in enumerate(local_copies)]

    def issue(k):
        for c in ring_copies(k):
            c.start()
        if k < n_gather and k % 3 == 0:
            core_copy(k // 3, 6, core).start()

    last = n_gather + 3

    def event(k):
        if k > 0:
            for c in ring_copies(k):
                c.wait_recv()
        if k < n_gather:
            for e in range(2):
                core_copy(k // 3, 2 * (k % 3) + e, core).start()
        if k == n_gather:
            for e, s in ((RIGHT, 1), (LEFT, 3)):
                lo = s * tok + e * h2
                rs_send[2, e] = (gsum[lo:lo + h2, :] + rs_recv[0, e].astype(F32)).astype(BF16)
        if k + 2 < last:
            issue(k + 2)

    def gathered(j):
        for piece in range(7):
            core_copy(j, piece, 1 - core).wait_recv()

    def project(j, n_tiles, dot, dst):
        i, _, g = tensors[j]
        bm = xbuf.shape[1]

        def load(t, slot):
            return pltpu.make_async_copy(g.at[i, pl.ds(pl.multiple_of(t * bm, bm), bm), :], xbuf.at[slot], in_sem.at[slot])

        load(0, 0).start()

        def step(t, carry):
            slot = lax.rem(t, 2)

            @pl.when(t + 1 < seq // bm)
            def _():
                load(t + 1, 1 - slot).start()

            load(t, slot).wait()

            def col(c, carry):
                cols = pl.ds(pl.multiple_of(c * 256, 256), 256)
                dst[pl.ds(pl.multiple_of(t * bm, bm), bm), cols] = dot(xbuf[slot], cols).astype(BF16)
                return carry

            return lax.fori_loop(0, n_tiles, col, carry)

        lax.fori_loop(0, seq // bm, step, 0)

    def project_x(j):
        project(j, wide // 256, lambda a, cols: jnp.dot(a, wcat[:, cols], preferred_element_type=F32), nat)

    def project_y(j):
        project(j, qw // 256, lambda a, cols: lax.dot_general(a, wo[cols, :], NT, preferred_element_type=F32), donat)

    bq = CORES * tok
    row_id = lax.broadcasted_iota(jnp.int32, (bq, bq), 0)
    col_id = lax.broadcasted_iota(jnp.int32, (bq, bq), 1)

    def attention(events):
        dk_acc[...] = jnp.zeros_like(dk_acc)
        dv_acc[...] = jnp.zeros_like(dv_acc)

        def head(h, carry):
            lanes = pl.ds(pl.multiple_of(h * hd, hd), hd)
            for i in range(seq // bq):
                rs = slice(i * bq, (i + 1) * bq)
                n_k = (i + 1) * bq
                q = nat[rs, lanes]
                do = donat[rs, lanes]
                k = nat[:n_k, qw:qw + hd]
                v = nat[:n_k, qw + hd:]
                s = lax.dot_general(q, k, NT, preferred_element_type=F32)
                diag = jnp.where(row_id >= col_id, s[:, i * bq:], -jnp.inf)
                s = diag if i == 0 else jnp.concatenate([s[:, :i * bq], diag], axis=1)
                m = jnp.max(s, axis=1, keepdims=True)
                p = jnp.exp((s - m) * scale)
                p = p * (1.0 / jnp.sum(p, axis=1, keepdims=True))
                pb = p.astype(BF16)
                o = jnp.dot(pb, v, preferred_element_type=F32).astype(BF16)
                onat[rs, lanes] = o
                dp = lax.dot_general(do, v, NT, preferred_element_type=F32)
                dd = jnp.sum(do.astype(F32) * o.astype(F32), axis=1, keepdims=True)
                ds = (p * (dp - dd)).astype(BF16)
                dnat[rs, lanes] = (jnp.dot(ds, k, preferred_element_type=F32) * scale).astype(BF16)
                dk_acc[:n_k, :] += lax.dot_general(ds, q, TN, preferred_element_type=F32)
                dv_acc[:n_k, :] += lax.dot_general(pb, do, TN, preferred_element_type=F32)
            for at, ev in events:
                @pl.when(h == at)
                def _(ev=ev):
                    event(ev)
            return carry

        lax.fori_loop(0, heads, head, 0)
        dnat[:, qw:qw + hd] = (dk_acc[...] * scale).astype(BF16)
        dnat[:, qw + hd:] = dv_acc[...].astype(BF16)

    def out_copies():
        return (pltpu.make_async_copy(dnat.at[:, pl.ds(0, qw)], dq_out, out_sem.at[0]),
                pltpu.make_async_copy(onat, o_out, out_sem.at[1]))

    hs = seq // 2

    def kv_copy(i, what):
        mine = kv_all.at[i, spot, pl.ds(pl.multiple_of(core * hs, hs), hs), :]
        theirs = kv_all.at[i, 1 - spot, pl.ds(pl.multiple_of(core * hs, hs), hs), :]
        give = kvp.at[pl.ds(pl.multiple_of((1 - core) * hs, hs), hs), :]
        src, dst, dev = ((give, kv_in.at[i], mate), (mine, mine, pair), (mine, mine, mate), (theirs, theirs, mate))[what]
        return remote(src, dst, kv_s.at[i, what], kv_r.at[i, what], dev)

    def kv_start(i):
        if i > 0:
            kv_copy(i - 1, 0).wait_send()
        kvp[:, :hd] = dk_acc[...] * scale
        kvp[:, hd:] = dv_acc[...]
        kv_copy(i, 0).start()

    def kv_sum(i):
        kv_copy(i, 0).wait_recv()
        at = pl.ds(pl.multiple_of(core * hs, hs), hs)
        kv_all[i, spot, at, :] = (kvp[at, :] + kv_in[i]).astype(BF16)
        kv_copy(i, 1).start()
        kv_copy(i, 2).start()

    def kv_forward(i):
        kv_copy(i, 1).wait_recv()
        kv_copy(i, 3).start()

    def kv_finish(i):
        kv_copy(i, 2).wait_recv()
        kv_copy(i, 3).wait_recv()

    n_mate = mate_stage.shape[0]
    bn = d // n_mate

    def mate_copy(i, c):
        return remote(mate_stage.at[c], mate_recv.at[i, c], mate_s.at[i, c], mate_r.at[i, c], mate)

    def pick(q):
        for s in range(chips):
            lhs[s * tok:(s + 1) * tok, :] = dnat[pl.ds(pl.multiple_of(block(s, q), tok), tok), :]

    def dx_share(i):
        pick(1 - core)
        for c in range(n_mate):
            if i > 0:
                mate_copy(i - 1, c).wait_send()

            def tile(t, carry, c=c):
                w = wcat[pl.ds(pl.multiple_of(c * bn + t * 256, 256), 256), :]
                cols = pl.ds(pl.multiple_of(t * 256, 256), 256)
                mate_stage[c, :, cols] = lax.dot_general(lhs[...], w, NT, preferred_element_type=F32).astype(BF16)
                return carry

            lax.fori_loop(0, bn // 256, tile, 0)
            mate_copy(i, c).start()
        kv_sum(i)
        pick(core)
        for c in range(n_mate):
            mate_copy(i, c).wait_recv()

            def tile(t, carry, c=c):
                cols = pl.ds(pl.multiple_of(c * bn + t * 256, 256), 256)
                got = mate_recv[i, c, :, pl.ds(pl.multiple_of(t * 256, 256), 256)]
                gsum[:, cols] = lax.dot_general(lhs[...], wcat[cols, :], NT, preferred_element_type=F32) + got.astype(F32)
                return carry

            lax.fori_loop(0, bn // 256, tile, 0)

    def wgrad(g, i, buf, put, dot):
        bt = tbuf.shape[2]
        tiles = d // bt

        def cols(t):
            return pl.ds(pl.multiple_of(t * bt, bt), bt)

        def load(t, slot):
            return pltpu.make_async_copy(g.at[i, :, cols(t)], tbuf.at[slot], tile_sem.at[0, slot])

        def save(t, slot):
            return pltpu.make_async_copy(buf.at[slot], put(cols(t)), tile_sem.at[1, slot])

        deep = tbuf.shape[0]
        for t in range(deep - 1):
            load(t, t).start()

        def step(t, carry):
            slot = lax.rem(t, deep)

            @pl.when(t + deep - 1 < tiles)
            def _():
                load(t + deep - 1, lax.rem(t + deep - 1, deep)).start()

            load(t, slot).wait()

            @pl.when(t >= deep)
            def _():
                save(t - deep, slot).wait()

            buf[slot] = dot(tbuf[slot])
            save(t, slot).start()
            return carry

        lax.fori_loop(0, tiles, step, 0)
        for t in range(tiles - deep, tiles):
            save(t, t % deep).wait()

    def half(s, e):
        return gsum[s * tok + e * h2:s * tok + (e + 1) * h2, :]

    kv_cols = pl.ds(pl.multiple_of(me // (n // kv_heads) * hd, hd), hd)
    loads = [pltpu.make_async_copy(wq_in, wcat.at[:, pl.ds(0, qw)], w_sem.at[0]),
             pltpu.make_async_copy(wk_in.at[:, kv_cols], wcat.at[:, pl.ds(qw, hd)], w_sem.at[1]),
             pltpu.make_async_copy(wv_in.at[:, kv_cols], wcat.at[:, pl.ds(qw + hd, hd)], w_sem.at[2]),
             pltpu.make_async_copy(wo_in, wo, w_sem.at[3])]
    issue(1)
    core_copy(0, 6, core).start()
    for c in to_vmem:
        c.start()
    for c in loads:
        c.start()
    event(0)
    for c, w in zip(to_vmem, to_hbm):
        c.wait()
        w.start()
    for k in range(1, 3):
        event(k)
    for c in to_hbm:
        c.wait()
    for c in loads:
        c.wait()
    gathered(0)
    project_x(0)
    for k in range(3, 6):
        event(k)
    gathered(1)
    project_y(1)
    attention(((0, 6), (3, 7)))
    kv_start(0)
    dx_share(0)
    for item, e, s, part in ((0, 0, 2, 0), (0, 1, 2, 1), (1, 0, 1, 1), (1, 1, 3, 0)):
        rs_send[item, e] = half(s, part).astype(BF16)
    dx_buf[...] = gsum[:tok, :]
    event(8)
    gathered(2)
    project_x(2)
    event(9)
    kv_forward(0)
    wgrad(xg, 0, qbuf, lambda cols: dwq_out.at[cols, :],
          lambda a: lax.dot_general(a, dnat[:, :qw], TN, preferred_element_type=F32))
    event(10)
    wgrad(yg, 0, obuf, lambda cols: dwo_out.at[:, cols],
          lambda a: lax.dot_general(onat[...], a, TN, preferred_element_type=F32))
    event(11)
    gathered(3)
    project_y(3)
    attention(((0, 12), (3, 13)))
    kv_start(1)
    for c in out_copies():
        c.start()
    dx_share(1)
    outs = []
    for item, (s, part, out) in enumerate(((2, 0, o0_out), (2, 1, o1_out), (1, 1, b1_out), (3, 0, c0_out))):
        snd_buf[item] = half(s, part).astype(BF16)
        outs.append(pltpu.make_async_copy(snd_buf.at[item], out, out_sem.at[2 + item]))
        outs[-1].start()
    for item, (lo, size, out) in enumerate(((tok, h2, r0_out), (3 * tok + h2, h2, l1_out), (0, tok, own_out))):
        outs.append(pltpu.make_async_copy(gsum.at[pl.ds(lo, size), :], out, out_sem.at[6 + item]))
        outs[-1].start()
    event(14)
    kv_forward(1)
    for c in ring_copies(n_gather):
        c.wait_send()
    lo = dx_buf[:h2, :] + rs_recv[2, RIGHT].astype(F32) + rs_recv[1, LEFT].astype(F32)
    hi = dx_buf[h2:, :] + rs_recv[1, RIGHT].astype(F32) + rs_recv[2, LEFT].astype(F32)
    rs_send[0, 0] = lo.astype(BF16)
    rs_send[0, 1] = hi.astype(BF16)
    fin = pltpu.make_async_copy(rs_send.at[0], dx_out, out_sem.at[9])
    fin.start()
    for i in range(micro_n):
        kv_finish(i)
    kv_save = pltpu.make_async_copy(kv_all, kv_out, out_sem.at[10])
    kv_save.start()
    for k in range(1, last):
        if k != n_gather:
            for c in ring_copies(k):
                c.wait_send()
    for j in range(len(tensors)):
        for piece in range(7):
            core_copy(j, piece, core).wait_send()
    for c in range(n_mate):
        mate_copy(1, c).wait_send()
    kv_copy(1, 0).wait_send()
    for i in range(micro_n):
        for what in range(1, 4):
            kv_copy(i, what).wait_send()
    kv_save.wait()
    for c in out_copies():
        c.wait()
    for c in outs:
        c.wait()
    fin.wait()


def fused(x, y, wq, wk, wv, wo, l0, r1, chips, heads, hd):
    micro_n, tok, d = x.shape
    h2 = tok // 2
    seq = chips * CORES * tok
    qw, wide = heads * hd, (heads + 2) * hd
    half = chips * tok
    n_mate = 4
    any_spec = pl.BlockSpec(memory_space=pl.ANY)
    items = 6 * micro_n + 3
    dma = pltpu.SemaphoreType.DMA
    part16, part32 = jax.ShapeDtypeStruct((h2, d), BF16), jax.ShapeDtypeStruct((h2, d), F32)
    return pl.pallas_call(
        functools.partial(fused_kernel, chips, heads, hd, wk.shape[1] // hd),
        out_shape=(jax.ShapeDtypeStruct((micro_n, seq, d), BF16), jax.ShapeDtypeStruct((micro_n, seq, d), BF16),
                   jax.ShapeDtypeStruct((seq, qw), BF16), jax.ShapeDtypeStruct((seq, qw), BF16),
                   jax.ShapeDtypeStruct((micro_n, 2, seq, 2 * hd), BF16), jax.ShapeDtypeStruct((2, h2, d), BF16),
                   part16, part16, part16, part16, part32, part32, jax.ShapeDtypeStruct((tok, d), F32),
                   jax.ShapeDtypeStruct((d, qw), F32), jax.ShapeDtypeStruct((qw, d), F32)),
        in_specs=[any_spec] * 8,
        out_specs=(any_spec,) * 15,
        scratch_shapes=[
            pltpu.VMEM((d, wide), BF16), pltpu.VMEM((qw, d), BF16),
            pltpu.VMEM((seq, wide), BF16), pltpu.VMEM((seq, qw), BF16),
            pltpu.VMEM((seq, wide), BF16), pltpu.VMEM((seq, qw), BF16),
            pltpu.VMEM((seq, hd), F32), pltpu.VMEM((seq, hd), F32),
            pltpu.VMEM((2, 256, d), BF16), pltpu.VMEM((half, wide), BF16), pltpu.VMEM((half, d), F32),
            pltpu.VMEM((n_mate, half, d // n_mate), BF16), pltpu.VMEM((micro_n, n_mate, half, d // n_mate), BF16),
            pltpu.VMEM((3, 2, h2, d), BF16), pltpu.VMEM((3, 2, h2, d), BF16),
            pltpu.VMEM((tok, d), F32), pltpu.VMEM((4, h2, d), BF16),
            pltpu.VMEM((seq, 2 * hd), F32), pltpu.VMEM((micro_n, seq // 2, 2 * hd), F32),
            pltpu.VMEM((micro_n, 2, seq, 2 * hd), BF16),
            pltpu.VMEM((4, seq, 256), BF16), pltpu.VMEM((4, 256, qw), F32), pltpu.VMEM((4, qw, 256), F32),
            dma((items, 2)), dma((items, 2)), dma((2 * micro_n, 7)), dma((2 * micro_n, 7)),
            dma((micro_n, n_mate)), dma((micro_n, n_mate)), dma((micro_n, 4)), dma((micro_n, 4)),
            dma((2, 2 * micro_n + 2)), dma((4,)), dma((2,)), dma((11,)), dma((2, 4))],
        compiler_params=pltpu.CompilerParams(collective_id=0, has_side_effects=True,
                                             vmem_limit_bytes=67043328),
        cost_estimate=pl.CostEstimate(flops=10 ** 11, bytes_accessed=2 ** 27, transcendentals=0),
        name="fused",
    )(x, y, wq, wk, wv, wo, l0, r1)


def wgrad_x_kernel(heads, hd, x, g, prev, dwq):
    out = prev[...] + lax.dot_general(x[...], g[...], TN, preferred_element_type=F32)
    for h in range(heads):
        dwq[pl.ds(h, out.shape[0], stride=heads), :] = out[:, h * hd:(h + 1) * hd]


def wgrad_x(x, g, prev, heads, hd):
    micro_n, seq, d = x.shape
    qw = g.shape[1]
    tile = 1024
    return pl.pallas_call(
        functools.partial(wgrad_x_kernel, heads, hd),
        grid=(d // tile,),
        out_shape=jax.ShapeDtypeStruct((d * heads, hd), F32),
        in_specs=[pl.BlockSpec((None, seq, tile), lambda i: (micro_n - 1, 0, i)),
                  pl.BlockSpec((seq, qw), lambda i: (0, 0)),
                  pl.BlockSpec((tile, qw), lambda i: (i, 0))],
        out_specs=pl.BlockSpec((tile * heads, hd), lambda i: (i, 0)),
        compiler_params=pltpu.CompilerParams(vmem_limit_bytes=62 * 2 ** 20),
        cost_estimate=pl.CostEstimate(flops=2 * seq * d * qw, bytes_accessed=2 ** 25, transcendentals=0),
        name="wgrad_x",
    )(x, g, prev).reshape(d, heads, hd)


def wgrad_kv_kernel(hd, _, x, kv, dwk, dwv):
    out = None
    for i in range(kv.shape[0]):
        for j in range(kv.shape[1]):
            term = lax.dot_general(x[i], kv[i, j], TN, preferred_element_type=F32)
            out = term if out is None else out + term
    dwk[...] = out[:, :hd]
    dwv[...] = out[:, hd:]


def wgrad_kv(x, kv, sub, group):
    micro_n, seq, d = x.shape
    hd = kv.shape[3] // 2
    tile = 512
    per = d // group // tile
    out = pl.BlockSpec((tile, hd), lambda i, at: (i, 0))
    return pl.pallas_call(
        functools.partial(wgrad_kv_kernel, hd),
        grid_spec=pltpu.PrefetchScalarGridSpec(
            num_scalar_prefetch=1, grid=(per,),
            in_specs=[pl.BlockSpec((micro_n, seq, tile), lambda i, at: (0, 0, at[0] * per + i)),
                      pl.BlockSpec(kv.shape, lambda i, at: (0, 0, 0, 0))],
            out_specs=(out, out)),
        out_shape=(jax.ShapeDtypeStruct((d // group, hd), F32),) * 2,
        compiler_params=pltpu.CompilerParams(vmem_limit_bytes=62 * 2 ** 20),
        cost_estimate=pl.CostEstimate(flops=8 * micro_n * seq * (d // group) * hd, bytes_accessed=2 ** 23,
                                      transcendentals=0),
        name="wgrad_kv",
    )(sub.reshape(1), x, kv)


def wgrad_o_kernel(o, y, prev, dwo):
    dwo[...] = prev[...] + lax.dot_general(o[...], y[...], TN, preferred_element_type=F32)


def wgrad_o(o, y, prev):
    micro_n, seq, d = y.shape
    qw = o.shape[1]
    tile = 1024
    out = pl.BlockSpec((qw, tile), lambda i: (0, i))
    return pl.pallas_call(
        wgrad_o_kernel,
        grid=(d // tile,),
        out_shape=jax.ShapeDtypeStruct((qw, d), F32),
        in_specs=[pl.BlockSpec((seq, qw), lambda i: (0, 0)),
                  pl.BlockSpec((None, seq, tile), lambda i: (micro_n - 1, 0, i)),
                  pl.BlockSpec((qw, tile), lambda i: (0, i))],
        out_specs=out,
        compiler_params=pltpu.CompilerParams(vmem_limit_bytes=62 * 2 ** 20),
        cost_estimate=pl.CostEstimate(flops=2 * seq * d * qw, bytes_accessed=2 ** 25, transcendentals=0),
        name="wgrad_o",
    )(o, y, prev)


def solution(mesh):
    n = mesh.shape["model"]
    chips = n // CORES
    right = [(i, (i + CORES) % n) for i in range(n)]
    left = [(i, (i - CORES) % n) for i in range(n)]

    def send(a, pairs):
        return lax.ppermute(a, "model", pairs)

    def device_grads(x_loc, dy_loc, w_q, w_k, w_v, w_o):
        micro_n, tok, d = x_loc.shape
        heads, hd = w_q.shape[1], w_q.shape[2]
        kv_heads = w_k.shape[1]
        group = n // kv_heads
        qw = heads * hd
        l0 = send(x_loc[0, :tok // 2], right)
        r1 = send(x_loc[0, tok // 2:], left)
        xg, yg, dq, o, kv, dx1, *tail = fused(
            x_loc, dy_loc, w_q.reshape(d, qw), w_k.reshape(d, kv_heads * hd), w_v.reshape(d, kv_heads * hd),
            w_o.reshape(qw, d), l0, r1, chips, heads, hd)
        o0, o1, b1, c0, r0, l1, own, dwq1, dwo1 = tail
        in_r0, in_l1 = send(o0, right), send(o1, left)
        b1, c0 = send(b1, right), send(c0, left)
        dwo = wgrad_o(o, yg, dwo1)
        dx = jnp.broadcast_to(dx1.reshape(1, tok, d), (micro_n, tok, d))
        in_r0, in_l1, dwo, dx = lax.optimization_barrier((in_r0, in_l1, dwo, dx))
        b0 = (r0 + in_r0.astype(F32)).astype(BF16)
        c1 = (l1 + in_l1.astype(F32)).astype(BF16)
        b0, c1, dq = lax.optimization_barrier((b0, c1, dq))
        b0, c1 = send(b0, right), send(c1, left)
        dwq = wgrad_x(xg, dq, dwq1, heads, hd)
        dwk, dwv = wgrad_kv(xg, kv, lax.axis_index("model") % group, group)
        from_left = jnp.concatenate([b0, b1]).astype(F32)
        from_right = jnp.concatenate([c0, c1]).astype(F32)
        dx2 = (own + from_left + from_right).astype(BF16)
        dx = lax.dynamic_update_slice(dx, dx2[None], (1, 0, 0))
        return (dx, dwq, dwk, dwv, dwo.reshape(heads, hd, d))

    return jax.shard_map(
        device_grads, mesh=mesh,
        in_specs=(P("data", "model", None), P("data", "model", None), P(None, "model", None),
                  P(None, None, None), P(None, None, None), P("model", None, None)),
        out_specs=(P("data", "model", None), P("data", "model", None), P(("data", "model"), None),
                   P(("data", "model"), None), P(("data", "model"), None, None)),
        check_vma=False)
```
